256 devices in a mesh: expert: 64 (over y, z, core), replica: 4 (over x).
Axes of the slice: x: 4, y: 4, z: 8, core: 2. Of those that a mesh axis runs over, the one named last changes fastest.
Arguments:
- tokens: bfloat16 [3072, 7168], P('expert', 'replica'), may hold values from -18 to 18
- expert_ids: int32 [3072, 8], P('expert'), may hold values from 0 to 63, all different within a row; in each aligned block of 48 rows (0 to 47, 48 to 95, ...) at most 12 rows name the same one
- route_weights: bfloat16 [3072, 8], P('expert'), may hold values from 0.1 to 1.5
- gate_weight: bfloat16 [64, 7168, 1024], P('expert', 'replica'), may hold values from -0.0625 to 0.0625
- up_weight: bfloat16 [64, 7168, 1024], P('expert', 'replica'), may hold values from -0.0625 to 0.0625
- down_weight: bfloat16 [64, 1024, 7168], P('expert', None, 'replica'), may hold values from -0.1875 to 0.1875
- bin_edges: float32 [16], replicated, may hold values from 0 to 20, as said below
Outputs:
- mixed: bfloat16 [3072, 7168], P('expert', 'replica')
- expert_load: float32 [64], P('expert')
The draws below stay inside these ranges and needn't reach their ends.
Inputs may be any that keep to these rules, and one draw needn't show every extreme that they name: `expert_ids`: each row names 8 different experts; within the 48 rows of one index of expert no expert is named by more than 12 rows, a bound that some block reaches. `bin_edges`: strictly increasing and positive; the last edge is 20, above every token entry's magnitude.
All inputs are finite; a program needn't handle non-finite values.
Results may differ from the reference program's by a relative error of at most 0.019.
Values may be sent and summed in bfloat16 or wider, within the bound.
No kernel may reach another device: no remote copies, remote signals or barrier semaphores. Data moves between devices by JAX's collectives and lax.ppermute only.
A program may use at most 128 MiB of HBM per device.

```python
import math
import jax
import jax.numpy as jnp
import numpy as np
from jax import lax

D = 7168
FF = 1024
TOP = 8
BINS = 16
FINE = 8
TOK_DEV = 48
EXPERTS = 64
CAP = 12
TOKENS = 3072
N_EXPERT = 64
N_REPLICA = 4


def draw_tokens(key, part):
    first = jax.random.fold_in(key, 11)
    second = jax.random.fold_in(key, 12)
    third = jax.random.fold_in(key, 13)
    channel_spread = jnp.exp(jax.random.uniform(second, (D,), jnp.float32, jnp.log(0.25), jnp.log(2.5)))
    row_spread = jnp.exp(jax.random.uniform(third, (TOKENS,), jnp.float32, jnp.log(0.5), jnp.log(1.2)))
    base = jnp.clip(jax.random.normal(first, (TOKENS, D), jnp.float32), -6.0, 6.0)
    return (base * channel_spread[None, :] * row_spread[:, None]).astype(jnp.bfloat16)


def draw_route_weights(key, part):
    blocks_all = TOKENS // TOK_DEV
    block_place = (jnp.arange(TOKENS, dtype=jnp.int32) // TOK_DEV).astype(jnp.float32)
    fraction = block_place / max(blocks_all - 1, 1)
    base = jax.random.uniform(jax.random.fold_in(key, 31), (TOKENS, TOP), jnp.float32, 0.1, 0.5)
    rising = 1.0 + 2.0 * fraction
    return (base * rising[:, None]).astype(jnp.bfloat16)


def draw_bin_edges(key, part):
    widths = jnp.exp(jax.random.uniform(jax.random.fold_in(key, 21), (BINS,), jnp.float32, jnp.log(0.5), jnp.log(2.0)))
    edges = 20.0 * jnp.cumsum(widths) / jnp.sum(widths)
    return edges.at[BINS - 1].set(20.0)


def shard_levels(rng, extent, shards, low, largest):
    gain, own = 1.0, jax.random.fold_in(rng, 6)
    for dim, shards_of in shards:
        steps = jnp.exp(jax.random.uniform(jax.random.fold_in(own, dim), (shards_of,), jnp.float32, low / len(shards), largest / len(shards)))
        gain = gain * jnp.repeat(steps, extent[dim] // shards_of).reshape([-1 if axis == dim else 1 for axis in range(len(extent))])
    return gain


def deal_out(stream_key, own, number, rows, count, top, most, skew):
    order = jax.random.permutation(stream_key, count)
    crowded, common = load_shares(count, rows * top, most, skew, True), load_shares(count, rows * top, most, skew, False)
    places = jnp.arange(count)

    def named(sizes, rotation):
        used = int((sizes > 0).sum())
        fixed = max(1, used // 4)
        passed = fixed + (places - fixed + rotation * (used - fixed)) % max(1, count - fixed)
        return jnp.zeros((count,), jnp.int32).at[order[jnp.where(places < fixed, places, passed)]].set(jnp.asarray(sizes, jnp.int32))

    sizes = jnp.where(number % 4 == 0, named(crowded, number // 4), named(common, number - number // 4 - 1))
    mixed = jax.random.permutation(jax.random.fold_in(own, 3), count)
    donor, taker = mixed[0:count // 2 * 2:2], mixed[1:count // 2 * 2:2]
    margin = jnp.minimum(sizes[donor] - 1, most - sizes[taker]) // 2
    margin = jnp.where((donor == order[0]) | (taker == order[0]) | (sizes[taker] == 0), 0, jnp.maximum(margin, 0))
    passed = jax.random.randint(jax.random.fold_in(own, 4), (count // 2,), 0, 1 << 20) % (margin + 1)
    sizes = sizes.at[donor].add(-passed).at[taker].add(passed)
    labels = jnp.searchsorted(jnp.cumsum(sizes), jnp.arange(rows * top), side="right").astype(jnp.int32)
    grid = labels.reshape(top, rows).T
    grid = grid[jax.random.permutation(jax.random.fold_in(own, 1), rows)]
    rotation = jax.random.randint(jax.random.fold_in(own, 2), (rows, 1), 0, top)
    return jnp.take_along_axis(grid, (jnp.arange(top)[None, :] + rotation) % top, axis=1)


def load_shares(count, total, reach, slope, full):
    portions = [(1 << 20) // math.isqrt(grade ** slope) + 1 for grade in range(1, count + 1)]
    largest = reach if full else min(reach, max(-(-total // count), total * portions[0] // sum(portions)))
    least = 1 if total - largest >= count - 1 else 0
    holding, rest = [largest] + [least] * (count - 1), total - largest - least * (count - 1)
    while rest > 0:
        free = [i for i in range(1, count) if holding[i] < largest] or [i for i in range(1, count) if holding[i] < reach]
        pool, budget = sum([portions[i] for i in free]), rest
        for i in free:
            addition = min(reach - holding[i], max(1, budget * portions[i] // pool), rest)
            holding[i] = holding[i] + addition
            rest = rest - addition
    return np.array(holding)


def bell_draw(key, extent, scale, reach, shards=(), kind=jnp.bfloat16):
    array = scale * jax.random.normal(key, extent, jnp.float32)
    if shards:
        array = array * shard_levels(key, extent, shards, -0.22, 0.18)
    return jnp.clip(array, -reach, reach).astype(kind)


def setup_inputs(seed: int = 0) -> dict:
    key_list = jax.random.split(jax.random.key(seed), 8)
    tokens = draw_tokens(jax.random.fold_in(key_list[7], 71), 0)
    expert_ids_keys = jax.random.split(jax.random.fold_in(key_list[1], 1), TOKENS // TOK_DEV)
    expert_ids_turns = jax.random.permutation(jax.random.fold_in(key_list[1], 3), TOKENS // TOK_DEV)
    expert_ids = jax.vmap(lambda own, number: deal_out(jax.random.fold_in(key_list[1], 2), own, number, TOK_DEV, EXPERTS, TOP, CAP, 2))(expert_ids_keys, expert_ids_turns).reshape((TOKENS, TOP))
    route_weights = draw_route_weights(jax.random.fold_in(key_list[7], 71), 0)
    gate_weight = bell_draw(key_list[3], (EXPERTS, D, FF), D ** -0.5, 0.0625, ((0, 64), (1, 4)))
    up_weight = bell_draw(key_list[4], (EXPERTS, D, FF), D ** -0.5, 0.0625, ((0, 64), (1, 4)))
    down_weight = bell_draw(key_list[5], (EXPERTS, FF, D), FF ** -0.5, 0.1875, ((0, 64), (2, 4)))
    bin_edges = draw_bin_edges(jax.random.fold_in(key_list[7], 71), 0)
    return {"tokens": tokens, "expert_ids": expert_ids, "route_weights": route_weights, "gate_weight": gate_weight, "up_weight": up_weight, "down_weight": down_weight, "bin_edges": bin_edges}


clip_parts = 8


def above_counts(magnitude, levels):
    return lax.map(lambda level: jnp.sum((magnitude >= level).astype(jnp.int32), axis=0), levels)


def clip_scales(magnitude, edges, limit):
    coarse = above_counts(magnitude, edges)
    chosen = jnp.sum((coarse > limit).astype(jnp.int32), axis=0)
    places = jnp.arange(edges.shape[0], dtype=jnp.int32)
    upper = jnp.sum(jnp.where(places[:, None] == chosen[None, :], edges[:, None], jnp.zeros_like(edges)[:, None]), axis=0)
    lower = jnp.sum(jnp.where(places[:, None] == chosen[None, :] - 1, edges[:, None], jnp.zeros_like(edges)[:, None]), axis=0)
    fractions = jnp.arange(1, FINE + 1).astype(edges.dtype) / FINE
    levels = lower[None, :] + (upper - lower)[None, :] * fractions[:, None]
    levels = jnp.concatenate([levels[:-1], upper[None, :]], axis=0)
    refined = above_counts(magnitude, levels)
    picked = jnp.sum((refined > limit).astype(jnp.int32), axis=0)
    steps = jnp.arange(FINE, dtype=jnp.int32)
    return jnp.sum(jnp.where(steps[:, None] == picked[None, :], levels, jnp.zeros_like(levels)), axis=0)


def reference(tokens, expert_ids, route_weights, gate_weight, up_weight, down_weight, bin_edges):
    slots = N_EXPERT * CAP
    share = D // N_REPLICA
    flat_ids = expert_ids.reshape(-1)
    blocks = expert_ids.reshape(N_EXPERT, TOK_DEV * TOP)
    hits = (blocks[:, :, None] == jnp.arange(EXPERTS, dtype=jnp.int32)[None, None, :]).astype(jnp.int32)
    ranks = jnp.sum((jnp.cumsum(hits, axis=1) - hits) * hits, axis=2)
    sources = jnp.arange(N_EXPERT, dtype=jnp.int32)[:, None]
    position = (sources * CAP + ranks).reshape(-1).astype(jnp.int32)
    owner = (jnp.arange(TOKENS * TOP, dtype=jnp.int32) // TOP).astype(jnp.int32)
    weights = route_weights.reshape(-1).astype(jnp.float32)
    padded = jnp.concatenate([tokens, jnp.zeros((1, D), tokens.dtype)], axis=0)
    block_weights = weights.reshape(N_EXPERT, TOK_DEV * TOP)
    weight_sums = jnp.sum(hits.astype(jnp.float32) * block_weights[:, :, None], axis=(0, 1))
    expert_load = weight_sums * EXPERTS / (TOKENS * TOP)

    def one_expert(total, inputs):
        gate_w, up_w, down_w, number = inputs
        match = flat_ids == number
        target = jnp.where(match, position, slots).astype(jnp.int32)
        row_owner = jnp.full((slots,), TOKENS, jnp.int32).at[target].set(owner, mode="drop")
        row_weight = jnp.zeros((slots,), jnp.float32).at[target].set(weights, mode="drop")
        rows = padded[row_owner]
        limit = jnp.sum(match.astype(jnp.int32)) // clip_parts
        scale = clip_scales(jnp.abs(rows), bin_edges, limit)
        quantized = (jnp.clip(rows.astype(jnp.float32), -scale, scale) / scale).astype(jnp.bfloat16)
        gate_fold = (gate_w.astype(jnp.float32) * scale[:, None]).astype(jnp.bfloat16)
        up_fold = (up_w.astype(jnp.float32) * scale[:, None]).astype(jnp.bfloat16)
        gate = jnp.zeros((slots, FF), jnp.float32)
        up_sum = jnp.zeros((slots, FF), jnp.float32)
        for block in range(N_REPLICA):
            low = block * share
            piece = quantized[:, low:low + share].astype(jnp.float32)
            gate_part = jnp.dot(piece, gate_fold[low:low + share].astype(jnp.float32), precision=lax.Precision.HIGHEST)
            up_part = jnp.dot(piece, up_fold[low:low + share].astype(jnp.float32), precision=lax.Precision.HIGHEST)
            gate = gate + lax.optimization_barrier(gate_part.astype(jnp.bfloat16)).astype(jnp.float32)
            up_sum = up_sum + lax.optimization_barrier(up_part.astype(jnp.bfloat16)).astype(jnp.float32)
        hidden = (jax.nn.silu(gate) * up_sum).astype(jnp.bfloat16)
        result = jnp.dot(hidden.astype(jnp.float32), down_w.astype(jnp.float32), precision=lax.Precision.HIGHEST)
        result = lax.optimization_barrier(result.astype(jnp.bfloat16)).astype(jnp.float32)
        total = total.at[row_owner].add(row_weight[:, None] * result, mode="drop")
        return total, None

    numbers = jnp.arange(EXPERTS, dtype=jnp.int32)
    total, _ = lax.scan(one_expert, jnp.zeros((TOKENS, D), jnp.float32), (gate_weight, up_weight, down_weight, numbers))
    return total.astype(jnp.bfloat16), expert_load
```

```python
import functools

import jax
import jax.numpy as jnp
import numpy as np
from jax import lax
from jax.experimental import pallas as pl
from jax.experimental.pallas import tpu as pltpu
from jax.sharding import Mesh
from jax.sharding import PartitionSpec as P


FINE = 8
CLIP_PARTS = 8
CAP = 12
META = 128
NY, NZ, NC, NX = 4, 8, 2, 4
PEERS = NY * NC
EXPERT = ("y", "z", "c")
OWNERS = ("y", "c")
GROUPS = ((0, 1, 7, 2, 6, 3, 5, 4),)

BF = jnp.bfloat16
F32 = jnp.float32
VMEM = pltpu.VMEM
SMEM = pltpu.SMEM


def whole(space=VMEM):
    return pl.BlockSpec(memory_space=space)


def lane_table(count):
    span = CAP * count
    lane = np.arange(PEERS * span)
    peer = lane // span
    table = np.zeros((8, PEERS * span), np.float32)
    table[0] = (peer // NC) * (NZ * NC) + peer % NC
    table[1] = (lane % span) // CAP
    table[2] = lane % CAP
    return table


def dispatch_kernel(count, others, z_ref, table_ref, *refs):
    blocks, extra = refs[:count], refs[count : count + others]
    rows_ref, combine_ref, map_ref, tokens_ref = refs[count + others :]
    tok, width = rows_ref.shape[2] and blocks[0].shape[0], rows_ref.shape[2]
    span = CAP * count
    lanes = PEERS * span
    z_part = (z_ref[0] * NC).astype(F32)
    expert = table_ref[0:1, :] + z_part
    place = table_ref[1:2, :]
    rank_wanted = table_ref[2:3, :]
    row = lax.broadcasted_iota(jnp.int32, (tok, tok), 0)
    col = lax.broadcasted_iota(jnp.int32, (tok, tok), 1)
    before = jnp.where(col < row, 1.0, 0.0).astype(BF)
    for i in range(count):
        meta = blocks[i][:, width : width + META].astype(F32)
        hit = jnp.zeros((tok, lanes), F32)
        weight = jnp.zeros((tok, lanes), F32)
        for k in range(8):
            same = meta[:, k : k + 1] == expert
            hit = jnp.where(same, 1.0, hit)
            weight = jnp.where(same, meta[:, 8 + k : 9 + k], weight)
        rank = jnp.dot(before, hit.astype(BF), preferred_element_type=F32)
        chosen = (hit > 0.0) & (rank == rank_wanted) & (place == float(i))
        map_ref[i * tok : (i + 1) * tok, :] = jnp.where(chosen, 1.0, 0.0).astype(BF)
        combine_ref[i * tok : (i + 1) * tok, :] = jnp.where(chosen, weight, 0.0).astype(BF)
        tokens_ref[i * tok : (i + 1) * tok, :] = blocks[i][:, :width]
    rows = lax.dot_general(
        map_ref[...], tokens_ref[...], (((0,), (0,)), ((), ())), preferred_element_type=F32
    ).astype(BF)
    for d in range(PEERS):
        rows_ref[d, 0:span, :] = rows[d * span : (d + 1) * span, :]
    if rows_ref.shape[1] > span:
        lane = lax.broadcasted_iota(jnp.int32, (1, META), 1)
        peer_expert = ((lane // NC) * (NZ * NC) + lane % NC).astype(F32) + z_part
        named = jnp.zeros((1, META), F32)
        load = jnp.zeros((1, META), F32)
        metas = [b[:, width : width + META] for b in blocks] + [b[...] for b in extra]
        for meta in metas:
            meta = meta.astype(F32)
            for k in range(8):
                same = meta[:, k : k + 1] == peer_expert
                named = named + jnp.sum(jnp.where(same, 1.0, 0.0), axis=0, keepdims=True)
                load = load + jnp.sum(
                    jnp.where(same, meta[:, 8 + k : 9 + k], 0.0), axis=0, keepdims=True
                )
        high = load.astype(BF).astype(F32)
        middle = (load - high).astype(BF).astype(F32)
        low = load - high - middle
        line = lax.broadcasted_iota(jnp.int32, (8, META), 0)
        pieces = jnp.where(
            line == 0, named, jnp.where(line == 1, high, jnp.where(line == 2, middle, jnp.where(line == 3, low, 0.0)))
        )
        for d in range(PEERS):
            rows_ref[d, span : span + 8, :] = jnp.broadcast_to(pieces[:, d : d + 1], (8, width)).astype(BF)


def dispatch(z, blocks, extra, last):
    count = len(blocks)
    tok, wide = blocks[0].shape
    width = wide - META
    span = CAP * count
    lanes = PEERS * span
    table = jnp.asarray(lane_table(count))
    side = pl.BlockSpec((tok, META), lambda i: (0, width // META))
    full = pl.BlockSpec((tok, wide), lambda i: (0, 0))
    tall = span + (8 if last else 0)
    return pl.pallas_call(
        functools.partial(dispatch_kernel, count, len(extra)),
        grid=(1,),
        in_specs=[whole(SMEM), pl.BlockSpec((8, lanes), lambda i: (0, 0))]
        + [full] * count
        + [side] * len(extra),
        out_specs=[
            pl.BlockSpec((PEERS, tall, width), lambda i: (0, 0, 0)),
            pl.BlockSpec((tok * count, lanes), lambda i: (0, 0)),
        ],
        out_shape=[
            jax.ShapeDtypeStruct((PEERS, tall, width), BF),
            jax.ShapeDtypeStruct((tok * count, lanes), BF),
        ],
        scratch_shapes=[VMEM((tok * count, lanes), BF), VMEM((tok * count, width), BF)],
        name="dispatch",
    )(z, table, *blocks, *extra)


STRIP = 256


def expert_kernel(spans, x_ref, edges_ref, gate_hbm, up_hbm, *refs):
    groups = len(spans)
    arrived = refs[:groups]
    outs = refs[groups : groups + 2 * NX * groups]
    load_ref = refs[groups + 2 * NX * groups]
    gate_ref, up_ref, clipped, sems = refs[groups + 2 * NX * groups + 1 :]
    width = clipped.shape[1]
    copies = [
        pltpu.make_async_copy(gate_hbm, gate_ref, sems.at[0]),
        pltpu.make_async_copy(up_hbm, up_ref, sems.at[1]),
    ]
    for copy in copies:
        copy.start()
    edges = [edges_ref[j] for j in range(16)]
    last, tail = arrived[-1], spans[-1]
    load = jnp.zeros((8, 128), F32)
    for d in range(PEERS):
        load = load + last[d, tail : tail + 8, 0:128].astype(F32)
    load_ref[...] = jnp.broadcast_to(load[1:2] + load[2:3] + load[3:4], (8, 128))

    def strip(s, carry):
        at = pl.ds(pl.multiple_of(s * STRIP, STRIP), STRIP)
        total = jnp.zeros((8, STRIP), F32)
        for d in range(PEERS):
            total = total + last[d, tail : tail + 8, at].astype(F32)
        limit = jnp.floor(total[0:1] / float(CLIP_PARTS))

        def more_above(level):
            near = level.astype(BF).astype(F32)
            above = (level * (1.0 + 2.0**-8)).astype(BF).astype(F32)
            bound = jnp.where(near >= level, near, above)
            bound = jnp.broadcast_to(bound, (16, STRIP)).astype(BF)
            count = jnp.zeros((16, STRIP), BF)
            for g in range(groups):
                for d in range(PEERS):
                    for r in range(0, spans[g], 16):
                        size = jnp.abs(arrived[g][d, r : r + 16, at])
                        count = count + jnp.where(size >= bound, jnp.ones_like(bound), jnp.zeros_like(bound))
            return jnp.sum(count.astype(F32), axis=0, keepdims=True) > limit

        def edge_at(place):
            value = jnp.zeros((1, STRIP), F32)
            for j in range(16):
                value = jnp.where(place == float(j), edges[j], value)
            return value

        m = jnp.zeros((1, STRIP), F32)
        for step in (8.0, 4.0, 2.0, 1.0):
            m = jnp.where(more_above(edge_at(m + (step - 1.0))), m + step, m)
        upper, lower = edge_at(m), edge_at(m - 1.0)
        n = jnp.zeros((1, STRIP), F32)
        for step in (4.0, 2.0, 1.0):
            level = lower + (upper - lower) * ((n + step) * (1.0 / FINE))
            n = jnp.where(more_above(level), n + step, n)
        scale = jnp.where(n == FINE - 1.0, upper, lower + (upper - lower) * ((n + 1.0) * (1.0 / FINE)))
        top = jnp.broadcast_to(scale, (16, STRIP)).astype(BF)
        base = 0
        for g in range(groups):
            for d in range(PEERS):
                for r in range(0, spans[g], 16):
                    clipped[base : base + 16, at] = jnp.minimum(
                        jnp.maximum(arrived[g][d, r : r + 16, at], -top), top
                    )
                    base += 16
        return carry

    lax.fori_loop(0, width // STRIP, strip, 0)
    for copy in copies:
        copy.wait()
    mine = x_ref[0]
    base = 0
    for g in range(groups):
        share = PEERS * spans[g] // NX
        for j in range(NX):
            at = pl.multiple_of(base + lax.rem(mine + j, NX) * share, 16)
            block = clipped[pl.ds(at, share), :]
            outs[2 * (NX * g + j)][...] = jnp.dot(
                block, gate_ref[...], preferred_element_type=F32
            ).astype(BF)
            outs[2 * (NX * g + j) + 1][...] = jnp.dot(
                block, up_ref[...], preferred_element_type=F32
            ).astype(BF)
        base += share * NX


def expert_in(x, edges, gate, up, arrived, spans):
    width, hidden = gate.shape
    shapes = []
    for span in spans:
        shapes += [jax.ShapeDtypeStruct((PEERS * span // NX, hidden), BF)] * (2 * NX)
    shapes.append(jax.ShapeDtypeStruct((8, 128), F32))
    outs = pl.pallas_call(
        functools.partial(expert_kernel, spans),
        in_specs=[whole(SMEM), whole(SMEM), whole(pl.ANY), whole(pl.ANY)] + [whole()] * len(spans),
        out_specs=[whole()] * len(shapes),
        out_shape=shapes,
        scratch_shapes=[
            VMEM((width, hidden), BF),
            VMEM((width, hidden), BF),
            VMEM((PEERS * sum(spans), width), BF),
            pltpu.SemaphoreType.DMA((2,)),
        ],
        name="expert_in",
    )(x, edges, gate, up, *arrived)
    pieces = outs[:-1]
    step = 2 * NX
    return [pieces[g * step : (g + 1) * step] for g in range(len(spans))], outs[-1]


def down_kernel(x_ref, down_ref, *refs):
    out_ref = refs[NX]
    share = refs[0].shape[0]
    for j in range(NX):
        at = pl.multiple_of(lax.rem(x_ref[0] + j, NX) * share, 16)
        out_ref[pl.ds(at, share), :] = jnp.dot(
            refs[j][...], down_ref[...], preferred_element_type=F32
        ).astype(BF)


def expert_out(x, down, pieces):
    share, _ = pieces[0].shape
    return pl.pallas_call(
        down_kernel,
        in_specs=[whole(SMEM)] + [whole()] * (1 + NX),
        out_specs=whole(),
        out_shape=jax.ShapeDtypeStruct((share * NX, down.shape[1]), BF),
        name="expert_out",
    )(x, down, *pieces)


def combine_kernel(count, combine_ref, back_ref, *outs):
    tok = outs[0].shape[0]
    for i in range(count):
        total = jnp.dot(
            combine_ref[i * tok : (i + 1) * tok, :], back_ref[...], preferred_element_type=F32
        )
        outs[i][...] = total.astype(BF)


def combined(combine, back, count):
    tok = combine.shape[0] // count
    return pl.pallas_call(
        functools.partial(combine_kernel, count),
        in_specs=[whole(), whole()],
        out_specs=[whole()] * count,
        out_shape=[jax.ShapeDtypeStruct((tok, back.shape[1]), BF)] * count,
        name="combine",
    )(combine, back)


def ring(value, axis, size, shift):
    if shift % size == 0:
        return value
    return lax.ppermute(value, axis, [(i, (i + shift) % size) for i in range(size)])


def body(tokens, expert_ids, route_weights, gate_weight, up_weight, down_weight, bin_edges):
    tok, width = tokens.shape
    z = lax.axis_index("z").astype(jnp.int32).reshape(1)
    x = lax.axis_index("x").astype(jnp.int32).reshape(1)
    side = jnp.concatenate([expert_ids.astype(BF), route_weights], axis=1)
    side = jnp.pad(side, ((0, 0), (0, META - side.shape[1])))
    wide = jnp.concatenate([tokens, side], axis=1)
    blocks = {o: ring(wide, "z", NZ, -o) for group in GROUPS for o in group}
    arrived, combines, spans = [], [], []
    for number, group in enumerate(GROUPS):
        last = number == len(GROUPS) - 1
        extra = [blocks[o] for other in GROUPS[:-1] for o in other] if last else []
        rows, combine = dispatch(z, [blocks[o] for o in group], extra, last)
        arrived.append(lax.all_to_all(rows, OWNERS, 0, 0, tiled=True))
        combines.append(combine)
        spans.append(CAP * len(group))
    partials, load = expert_in(x, bin_edges, gate_weight[0], up_weight[0], arrived, tuple(spans))
    expert_load = load[0, 0:1] / (tok * expert_ids.shape[1])
    total = None
    for number in reversed(range(len(GROUPS))):
        group, pieces = GROUPS[number], partials[number]
        gates, ups = pieces[0::2], pieces[1::2]
        far_gate = ring(gates[2], "x", NX, 1)
        far_up = ring(ups[2], "x", NX, -1)
        near_up = ring(ups[1], "x", NX, 1)
        near_gate = ring(gates[3], "x", NX, -1)
        sum_gate = (gates[1].astype(F32) + far_gate.astype(F32)).astype(BF)
        sum_up = (ups[3].astype(F32) + far_up.astype(F32)).astype(BF)
        right_gate = ring(sum_gate, "x", NX, 1)
        left_up = ring(sum_up, "x", NX, -1)
        gate = gates[0].astype(F32) + right_gate.astype(F32) + near_gate.astype(F32)
        up = ups[0].astype(F32) + near_up.astype(F32) + left_up.astype(F32)
        hidden = (jax.nn.silu(gate) * up).astype(BF)
        shares = [ring(hidden, "x", NX, -j) for j in range(NX)]
        result = expert_out(x, down_weight[0], shares)
        result = result.reshape(PEERS, spans[number], width)
        back = lax.all_to_all(result, OWNERS, 0, 0, tiled=True).reshape(-1, width)
        sums = combined(combines[number], back, len(group))
        for o, part in zip(group, sums):
            part = ring(part, "z", NZ, o).astype(F32)
            total = part if total is None else total + part
    return (total.astype(BF), expert_load)


def solution(mesh):
    finer = Mesh(mesh.devices.reshape(NY, NZ, NC, NX), ("y", "z", "c", "x"))
    placed = (
        P(EXPERT, "x"),
        P(EXPERT, None),
        P(EXPERT, None),
        P(EXPERT, "x", None),
        P(EXPERT, "x", None),
        P(EXPERT, None, "x"),
        P(),
    )
    return jax.shard_map(
        body,
        mesh=finer,
        in_specs=placed,
        out_specs=(P(EXPERT, "x"), P(EXPERT)),
        check_vma=False,
    )
```

```python
import functools

import jax
import jax.numpy as jnp
import numpy as np
from jax import lax
from jax.experimental import pallas as pl
from jax.experimental.pallas import tpu as pltpu
from jax.sharding import Mesh
from jax.sharding import PartitionSpec as P


FINE = 8
CLIP_PARTS = 8
CAP = 12
META = 128
NY, NZ, NC, NX = 4, 8, 2, 4
PEERS = NY * NC
EXPERT = ("y", "z", "c")
OWNERS = ("y", "c")
GROUPS = ((0, 1, 7, 2), (6, 3, 5, 4))

BF = jnp.bfloat16
F32 = jnp.float32
VMEM = pltpu.VMEM
SMEM = pltpu.SMEM


def whole(space=VMEM):
    return pl.BlockSpec(memory_space=space)


def lane_table(count):
    span = CAP * count
    lane = np.arange(PEERS * span)
    peer = lane // span
    table = np.zeros((8, PEERS * span), np.float32)
    table[0] = (peer // NC) * (NZ * NC) + peer % NC
    table[1] = (lane % span) // CAP
    table[2] = lane % CAP
    return table


def dispatch_kernel(count, others, z_ref, table_ref, *refs):
    blocks, extra = refs[:count], refs[count : count + others]
    rows_ref, combine_ref, map_ref, tokens_ref = refs[count + others :]
    tok, width = rows_ref.shape[2] and blocks[0].shape[0], rows_ref.shape[2]
    span = CAP * count
    lanes = PEERS * span
    z_part = (z_ref[0] * NC).astype(F32)
    expert = table_ref[0:1, :] + z_part
    place = table_ref[1:2, :]
    rank_wanted = table_ref[2:3, :]
    row = lax.broadcasted_iota(jnp.int32, (tok, tok), 0)
    col = lax.broadcasted_iota(jnp.int32, (tok, tok), 1)
    before = jnp.where(col < row, 1.0, 0.0).astype(BF)
    for i in range(count):
        meta = blocks[i][:, width : width + META].astype(F32)
        hit = jnp.zeros((tok, lanes), F32)
        weight = jnp.zeros((tok, lanes), F32)
        for k in range(8):
            same = meta[:, k : k + 1] == expert
            hit = jnp.where(same, 1.0, hit)
            weight = jnp.where(same, meta[:, 8 + k : 9 + k], weight)
        rank = jnp.dot(before, hit.astype(BF), preferred_element_type=F32)
        chosen = (hit > 0.0) & (rank == rank_wanted) & (place == float(i))
        map_ref[i * tok : (i + 1) * tok, :] = jnp.where(chosen, 1.0, 0.0).astype(BF)
        combine_ref[i * tok : (i + 1) * tok, :] = jnp.where(chosen, weight, 0.0).astype(BF)
        tokens_ref[i * tok : (i + 1) * tok, :] = blocks[i][:, :width]
    rows = lax.dot_general(
        map_ref[...], tokens_ref[...], (((0,), (0,)), ((), ())), preferred_element_type=F32
    ).astype(BF)
    for d in range(PEERS):
        rows_ref[d, 0:span, :] = rows[d * span : (d + 1) * span, :]
    if rows_ref.shape[1] > span:
        lane = lax.broadcasted_iota(jnp.int32, (1, META), 1)
        peer_expert = ((lane // NC) * (NZ * NC) + lane % NC).astype(F32) + z_part
        named = jnp.zeros((1, META), F32)
        load = jnp.zeros((1, META), F32)
        metas = [b[:, width : width + META] for b in blocks] + [b[...] for b in extra]
        for meta in metas:
            meta = meta.astype(F32)
            for k in range(8):
                same = meta[:, k : k + 1] == peer_expert
                named = named + jnp.sum(jnp.where(same, 1.0, 0.0), axis=0, keepdims=True)
                load = load + jnp.sum(
                    jnp.where(same, meta[:, 8 + k : 9 + k], 0.0), axis=0, keepdims=True
                )
        high = load.astype(BF).astype(F32)
        middle = (load - high).astype(BF).astype(F32)
        low = load - high - middle
        line = lax.broadcasted_iota(jnp.int32, (8, META), 0)
        pieces = jnp.where(
            line == 0, named, jnp.where(line == 1, high, jnp.where(line == 2, middle, jnp.where(line == 3, low, 0.0)))
        )
        for d in range(PEERS):
            rows_ref[d, span : span + 8, :] = jnp.broadcast_to(pieces[:, d : d + 1], (8, width)).astype(BF)


def dispatch(z, blocks, extra, last):
    count = len(blocks)
    tok, wide = blocks[0].shape
    width = wide - META
    span = CAP * count
    lanes = PEERS * span
    table = jnp.asarray(lane_table(count))
    side = pl.BlockSpec((tok, META), lambda i: (0, width // META))
    full = pl.BlockSpec((tok, wide), lambda i: (0, 0))
    tall = span + (8 if last else 0)
    return pl.pallas_call(
        functools.partial(dispatch_kernel, count, len(extra)),
        grid=(1,),
        in_specs=[whole(SMEM), pl.BlockSpec((8, lanes), lambda i: (0, 0))]
        + [full] * count
        + [side] * len(extra),
        out_specs=[
            pl.BlockSpec((PEERS, tall, width), lambda i: (0, 0, 0)),
            pl.BlockSpec((tok * count, lanes), lambda i: (0, 0)),
        ],
        out_shape=[
            jax.ShapeDtypeStruct((PEERS, tall, width), BF),
            jax.ShapeDtypeStruct((tok * count, lanes), BF),
        ],
        scratch_shapes=[VMEM((tok * count, lanes), BF), VMEM((tok * count, width), BF)],
        name="dispatch",
    )(z, table, *blocks, *extra)


STRIP = 256


def expert_kernel(spans, x_ref, edges_ref, gate_hbm, up_hbm, *refs):
    groups = len(spans)
    arrived = refs[:groups]
    outs = refs[groups : groups + 2 * NX * groups]
    load_ref = refs[groups + 2 * NX * groups]
    gate_ref, up_ref, clipped, sems = refs[groups + 2 * NX * groups + 1 :]
    width = clipped.shape[1]
    copies = [
        pltpu.make_async_copy(gate_hbm, gate_ref, sems.at[0]),
        pltpu.make_async_copy(up_hbm, up_ref, sems.at[1]),
    ]
    for copy in copies:
        copy.start()
    edges = [edges_ref[j] for j in range(16)]
    last, tail = arrived[-1], spans[-1]
    load = jnp.zeros((8, 128), F32)
    for d in range(PEERS):
        load = load + last[d, tail : tail + 8, 0:128].astype(F32)
    load_ref[...] = jnp.broadcast_to(load[1:2] + load[2:3] + load[3:4], (8, 128))

    def strip(s, carry):
        at = pl.ds(pl.multiple_of(s * STRIP, STRIP), STRIP)
        total = jnp.zeros((8, STRIP), F32)
        for d in range(PEERS):
            total = total + last[d, tail : tail + 8, at].astype(F32)
        limit = jnp.floor(total[0:1] / float(CLIP_PARTS))

        def more_above(level):
            near = level.astype(BF).astype(F32)
            above = (level * (1.0 + 2.0**-8)).astype(BF).astype(F32)
            bound = jnp.where(near >= level, near, above)
            bound = jnp.broadcast_to(bound, (16, STRIP)).astype(BF)
            count = jnp.zeros((16, STRIP), BF)
            for g in range(groups):
                for d in range(PEERS):
                    for r in range(0, spans[g], 16):
                        size = jnp.abs(arrived[g][d, r : r + 16, at])
                        count = count + jnp.where(size >= bound, jnp.ones_like(bound), jnp.zeros_like(bound))
            return jnp.sum(count.astype(F32), axis=0, keepdims=True) > limit

        def edge_at(place):
            value = jnp.zeros((1, STRIP), F32)
            for j in range(16):
                value = jnp.where(place == float(j), edges[j], value)
            return value

        m = jnp.zeros((1, STRIP), F32)
        for step in (8.0, 4.0, 2.0, 1.0):
            m = jnp.where(more_above(edge_at(m + (step - 1.0))), m + step, m)
        upper, lower = edge_at(m), edge_at(m - 1.0)
        n = jnp.zeros((1, STRIP), F32)
        for step in (4.0, 2.0, 1.0):
            level = lower + (upper - lower) * ((n + step) * (1.0 / FINE))
            n = jnp.where(more_above(level), n + step, n)
        scale = jnp.where(n == FINE - 1.0, upper, lower + (upper - lower) * ((n + 1.0) * (1.0 / FINE)))
        top = jnp.broadcast_to(scale, (16, STRIP)).astype(BF)
        base = 0
        for g in range(groups):
            share = PEERS * spans[g] // NX
            for d in range(PEERS):
                turn = lax.rem(d * NX // PEERS - x_ref[0] + NX, NX)
                start = base + turn * share + d % (PEERS // NX) * spans[g]
                for r in range(0, spans[g], 16):
                    clipped[pl.ds(pl.multiple_of(start + r, 16), 16), at] = jnp.minimum(
                        jnp.maximum(arrived[g][d, r : r + 16, at], -top), top
                    )
            base += PEERS * spans[g]
        return carry

    lax.fori_loop(0, width // STRIP, strip, 0)
    for copy in copies:
        copy.wait()
    base = PEERS * sum(spans)
    for g in reversed(range(groups)):
        share = PEERS * spans[g] // NX
        base -= share * NX
        block = clipped[base : base + share * NX, :]
        for side, weight in enumerate((gate_ref, up_ref)):
            product = jnp.dot(block, weight[...], preferred_element_type=F32).astype(BF)
            for j in range(NX):
                outs[2 * (NX * g + j) + side][...] = product[j * share : (j + 1) * share, :]


def expert_in(x, edges, gate, up, arrived, spans):
    width, hidden = gate.shape
    shapes = []
    for span in spans:
        shapes += [jax.ShapeDtypeStruct((PEERS * span // NX, hidden), BF)] * (2 * NX)
    shapes.append(jax.ShapeDtypeStruct((8, 128), F32))
    outs = pl.pallas_call(
        functools.partial(expert_kernel, spans),
        in_specs=[whole(SMEM), whole(SMEM), whole(pl.ANY), whole(pl.ANY)] + [whole()] * len(spans),
        out_specs=[whole()] * len(shapes),
        out_shape=shapes,
        scratch_shapes=[
            VMEM((width, hidden), BF),
            VMEM((width, hidden), BF),
            VMEM((PEERS * sum(spans), width), BF),
            pltpu.SemaphoreType.DMA((2,)),
        ],
        name="expert_in",
    )(x, edges, gate, up, *arrived)
    pieces = outs[:-1]
    step = 2 * NX
    return [pieces[g * step : (g + 1) * step] for g in range(len(spans))], outs[-1]


def down_kernel(x_ref, down_ref, *refs):
    out_ref, all_ref = refs[NX:]
    share = refs[0].shape[0]
    for j in range(NX):
        at = pl.multiple_of(lax.rem(x_ref[0] + j, NX) * share, 16)
        all_ref[pl.ds(at, share), :] = refs[j][...]
    out_ref[...] = jnp.dot(all_ref[...], down_ref[...], preferred_element_type=F32).astype(BF)


def expert_out(x, down, pieces):
    share, _ = pieces[0].shape
    return pl.pallas_call(
        down_kernel,
        in_specs=[whole(SMEM)] + [whole()] * (1 + NX),
        out_specs=whole(),
        out_shape=jax.ShapeDtypeStruct((share * NX, down.shape[1]), BF),
        scratch_shapes=[VMEM((share * NX, down.shape[0]), BF)],
        name="expert_out",
    )(x, down, *pieces)


def combine_kernel(count, combine_ref, back_ref, *outs):
    tok = outs[0].shape[0]
    total = jnp.dot(combine_ref[...], back_ref[...], preferred_element_type=F32).astype(BF)
    for i in range(count):
        outs[i][...] = total[i * tok : (i + 1) * tok, :]


def combined(combine, back, count):
    tok = combine.shape[0] // count
    return pl.pallas_call(
        functools.partial(combine_kernel, count),
        in_specs=[whole(), whole()],
        out_specs=[whole()] * count,
        out_shape=[jax.ShapeDtypeStruct((tok, back.shape[1]), BF)] * count,
        name="combine",
    )(combine, back)


def ring(value, axis, size, shift):
    if shift % size == 0:
        return value
    return lax.ppermute(value, axis, [(i, (i + shift) % size) for i in range(size)])


def body(tokens, expert_ids, route_weights, gate_weight, up_weight, down_weight, bin_edges):
    tok, width = tokens.shape
    z = lax.axis_index("z").astype(jnp.int32).reshape(1)
    x = lax.axis_index("x").astype(jnp.int32).reshape(1)
    side = jnp.concatenate([expert_ids.astype(BF), route_weights], axis=1)
    side = jnp.pad(side, ((0, 0), (0, META - side.shape[1])))
    wide = jnp.concatenate([tokens, side], axis=1)
    blocks = {}
    for group in GROUPS:
        for o in group:
            blocks[o] = ring(wide, "z", NZ, -o)
    arrived, combines, spans = [], [], []
    for number, group in enumerate(GROUPS):
        last = number == len(GROUPS) - 1
        extra = [blocks[o] for other in GROUPS[:-1] for o in other] if last else []
        rows, combine = dispatch(z, [blocks[o] for o in group], extra, last)
        arrived.append(lax.all_to_all(rows, OWNERS, 0, 0, tiled=True))
        combines.append(combine)
        spans.append(CAP * len(group))
    partials, load = expert_in(x, bin_edges, gate_weight[0], up_weight[0], arrived, tuple(spans))
    expert_load = load[0, 0:1] / (tok * expert_ids.shape[1])
    total = None
    for number in reversed(range(len(GROUPS))):
        group, pieces = GROUPS[number], partials[number]
        gates, ups = pieces[0::2], pieces[1::2]
        far_gate = ring(gates[2], "x", NX, 1)
        far_up = ring(ups[2], "x", NX, -1)
        near_up = ring(ups[1], "x", NX, 1)
        near_gate = ring(gates[3], "x", NX, -1)
        sum_gate = (gates[1].astype(F32) + far_gate.astype(F32)).astype(BF)
        sum_up = (ups[3].astype(F32) + far_up.astype(F32)).astype(BF)
        right_gate = ring(sum_gate, "x", NX, 1)
        left_up = ring(sum_up, "x", NX, -1)
        gate = gates[0].astype(F32) + right_gate.astype(F32) + near_gate.astype(F32)
        up = ups[0].astype(F32) + near_up.astype(F32) + left_up.astype(F32)
        hidden = (jax.nn.silu(gate) * up).astype(BF)
        shares = [ring(hidden, "x", NX, -j) for j in range(NX)]
        result = expert_out(x, down_weight[0], shares)
        result = result.reshape(PEERS, spans[number], width)
        back = lax.all_to_all(result, OWNERS, 0, 0, tiled=True).reshape(-1, width)
        sums = combined(combines[number], back, len(group))
        sums = [ring(part, "z", NZ, o) for o, part in zip(group, sums)]
        for part in sums:
            total = part.astype(F32) if total is None else total + part.astype(F32)
    return (total.astype(BF), expert_load)


def solution(mesh):
    finer = Mesh(mesh.devices.reshape(NY, NZ, NC, NX), ("y", "z", "c", "x"))
    placed = (
        P(EXPERT, "x"),
        P(EXPERT, None),
        P(EXPERT, None),
        P(EXPERT, "x", None),
        P(EXPERT, "x", None),
        P(EXPERT, None, "x"),
        P(),
    )
    return jax.shard_map(
        body,
        mesh=finer,
        in_specs=placed,
        out_specs=(P(EXPERT, "x"), P(EXPERT)),
        check_vma=False,
    )
```

```python
import functools

import jax
import jax.numpy as jnp
import numpy as np
from jax import lax
from jax.experimental import pallas as pl
from jax.experimental.pallas import tpu as pltpu
from jax.sharding import Mesh
from jax.sharding import PartitionSpec as P


FINE = 8
CLIP_PARTS = 8
CAP = 12
META = 128
NY, NZ, NC, NX = 4, 8, 2, 4
PEERS = NY * NC
EXPERT = ("y", "z", "c")
OWNERS = ("y", "c")
NEAR = ((0, 1), (7, 2))
FAR = ((6, 3), (5, 4))
PAIR = 2
SPAN = CAP * PAIR
LANES = PEERS * SPAN
HALF = SPAN * PAIR
ROWS = PEERS * HALF
SHARE = ROWS // NX
STRIP = 256
WIDE = 512

BF = jnp.bfloat16
F32 = jnp.float32
VMEM = pltpu.VMEM
SMEM = pltpu.SMEM


def whole(space=VMEM):
    return pl.BlockSpec(memory_space=space)


def shape_of(*shape):
    return jax.ShapeDtypeStruct(shape, BF)


def lane_table():
    lane = np.arange(LANES)
    table = np.zeros((8, LANES), np.float32)
    table[0] = lane // SPAN // NC
    table[1] = lane // SPAN % NC
    table[2] = lane % SPAN // CAP
    table[3] = lane % CAP
    return table


def peer(place, k, sign):
    dy, dc = k // NC, k % NC
    core = place[3] if dc == 0 else 1 - place[3]
    return lax.rem(place[1] + sign * dy + NY, NY) * NC + core


def dispatch_kernel(relative, place_ref, table_ref, *refs):
    tok = refs[0].shape[0]
    width = refs[0].shape[1] - META
    blocks = refs[: 2 * PAIR]
    extra = refs[2 * PAIR : 2 * PAIR + (2 * PAIR if relative else 0)]
    outs = refs[len(blocks) + len(extra) :]
    rows_refs, combine_refs, (map_ref, tokens_ref) = outs[:-4], outs[-4:-2], outs[-2:]

    def numbers(y, core):
        if relative:
            y = y + place_ref[1].astype(F32)
            y = jnp.where(y >= float(NY), y - float(NY), y)
            own = place_ref[3].astype(F32)
            core = own + core - 2.0 * own * core
        return y * float(NZ * NC) + core + place_ref[2].astype(F32) * float(NC)

    expert = numbers(table_ref[0:1, :], table_ref[1:2, :])
    spot = table_ref[2:3, :]
    rank_wanted = table_ref[3:4, :]
    row = lax.broadcasted_iota(jnp.int32, (tok, tok), 0)
    col = lax.broadcasted_iota(jnp.int32, (tok, tok), 1)
    before = jnp.where(col < row, 1.0, 0.0).astype(BF)
    for s in range(2):
        for i in range(PAIR):
            block = blocks[PAIR * s + i]
            meta = block[:, width : width + META].astype(F32)
            hit = jnp.zeros((tok, LANES), F32)
            weight = jnp.zeros((tok, LANES), F32)
            for k in range(8):
                same = meta[:, k : k + 1] == expert
                hit = jnp.where(same, 1.0, hit)
                weight = jnp.where(same, meta[:, 8 + k : 9 + k], weight)
            rank = jnp.dot(before, hit.astype(BF), preferred_element_type=F32)
            chosen = (hit > 0.0) & (rank == rank_wanted) & (spot == float(i))
            map_ref[i * tok : (i + 1) * tok, :] = jnp.where(chosen, 1.0, 0.0).astype(BF)
            combine_refs[s][i * tok : (i + 1) * tok, :] = jnp.where(chosen, weight, 0.0).astype(BF)
            tokens_ref[i * tok : (i + 1) * tok, :] = block[:, :width]
        rows = lax.dot_general(
            map_ref[...], tokens_ref[...], (((0,), (0,)), ((), ())), preferred_element_type=F32
        )
        for d in range(PEERS):
            part = rows[d * SPAN : (d + 1) * SPAN, :].astype(BF)
            if relative:
                rows_refs[d][s * SPAN : (s + 1) * SPAN, :] = part
            else:
                rows_refs[0][d, s * SPAN : (s + 1) * SPAN, :] = part
    if relative:
        lane = lax.broadcasted_iota(jnp.int32, (1, META), 1)
        peer_expert = numbers((lane // NC).astype(F32), (lane % NC).astype(F32))
        named = jnp.zeros((1, META), F32)
        load = jnp.zeros((1, META), F32)
        metas = [b[:, width : width + META] for b in blocks] + [b[...] for b in extra]
        for meta in metas:
            meta = meta.astype(F32)
            for k in range(8):
                same = meta[:, k : k + 1] == peer_expert
                named = named + jnp.sum(jnp.where(same, 1.0, 0.0), axis=0, keepdims=True)
                load = load + jnp.sum(
                    jnp.where(same, meta[:, 8 + k : 9 + k], 0.0), axis=0, keepdims=True
                )
        high = load.astype(BF).astype(F32)
        middle = (load - high).astype(BF).astype(F32)
        low = load - high - middle
        line = lax.broadcasted_iota(jnp.int32, (8, META), 0)
        pieces = jnp.where(line == 2, middle, jnp.where(line == 3, low, 0.0))
        pieces = jnp.where(line == 0, named, jnp.where(line == 1, high, pieces))
        for d in range(PEERS):
            rows_refs[d][HALF : HALF + 8, :] = jnp.broadcast_to(pieces[:, d : d + 1], (8, width)).astype(BF)


def dispatch(place, blocks, extra):
    tok, wide = blocks[0].shape
    width = wide - META
    side = pl.BlockSpec((tok, META), lambda i: (0, width // META))
    full = pl.BlockSpec((tok, wide), lambda i: (0, 0))
    flat = pl.BlockSpec((PAIR * tok, LANES), lambda i: (0, 0))
    if extra:
        specs = [pl.BlockSpec((HALF + 8, width), lambda i: (0, 0))] * PEERS
        shapes = [shape_of(HALF + 8, width)] * PEERS
    else:
        specs = [pl.BlockSpec((PEERS, HALF, width), lambda i: (0, 0, 0))]
        shapes = [shape_of(PEERS, HALF, width)]
    outs = pl.pallas_call(
        functools.partial(dispatch_kernel, bool(extra)),
        grid=(1,),
        in_specs=[whole(SMEM), pl.BlockSpec((8, LANES), lambda i: (0, 0))]
        + [full] * len(blocks)
        + [side] * len(extra),
        out_specs=specs + [flat] * 2,
        out_shape=shapes + [shape_of(PAIR * tok, LANES)] * 2,
        scratch_shapes=[VMEM((PAIR * tok, LANES), BF), VMEM((PAIR * tok, width), BF)],
        name="dispatch",
    )(place, jnp.asarray(lane_table()), *blocks, *extra)
    return outs[:-2], outs[-2:]


def products(block_ref, gate_ref, up_ref, outs):
    right, left, gate_own, up_own, gate_next, up_last = outs

    def columns(n, carry):
        at = pl.ds(pl.multiple_of(n * WIDE, WIDE), WIDE)
        gate = jnp.dot(block_ref[...], gate_ref[:, at], preferred_element_type=F32).astype(BF)
        right[:SHARE, at] = gate[2 * SHARE : 3 * SHARE, :]
        left[SHARE:, at] = gate[3 * SHARE :, :]
        gate_own[:, at] = gate[:SHARE, :]
        gate_next[:, at] = gate[SHARE : 2 * SHARE, :]
        up = jnp.dot(block_ref[...], up_ref[:, at], preferred_element_type=F32).astype(BF)
        left[:SHARE, at] = up[2 * SHARE : 3 * SHARE, :]
        right[SHARE:, at] = up[SHARE : 2 * SHARE, :]
        up_own[:, at] = up[:SHARE, :]
        up_last[:, at] = up[3 * SHARE :, :]
        return carry

    lax.fori_loop(0, gate_ref.shape[1] // WIDE, columns, 0)


def product_shapes(hidden):
    return [shape_of(2 * SHARE, hidden)] * 2 + [shape_of(SHARE, hidden)] * 4


def fetch(gate_hbm, up_hbm, gate_ref, up_ref, sems):
    return [
        pltpu.make_async_copy(gate_hbm, gate_ref, sems.at[0]),
        pltpu.make_async_copy(up_hbm, up_ref, sems.at[1]),
    ]


def expert_kernel(count, place_ref, edges_ref, gate_hbm, up_hbm, near_ref, *refs):
    far = refs[:PEERS]
    outs = refs[PEERS : PEERS + 6]
    near_clipped, load_ref = refs[PEERS + 6 : PEERS + 8]
    gate_ref, up_ref, far_clipped, sems = refs[PEERS + 8 :]
    width = far_clipped.shape[1]
    copies = fetch(gate_hbm, up_hbm, gate_ref, up_ref, sems)
    for copy in copies:
        copy.start()
    edges = [edges_ref[j] for j in range(16)]
    load = jnp.zeros((8, 128), F32)
    for k in range(PEERS):
        load = load + far[k][HALF : HALF + 8, 0:128].astype(F32)
    load = (load[1:2] + load[2:3] + load[3:4]) / float(count)
    load_ref[0] = load[0, 0]

    def home(d):
        turn = lax.rem(d // NC - place_ref[0] + NX, NX)
        return turn * SHARE + lax.rem(d, NC) * HALF

    near_home = [home(d) for d in range(PEERS)]
    far_home = [home(peer(place_ref, k, -1)) for k in range(PEERS)]

    def strip(s, carry):
        at = pl.ds(pl.multiple_of(s * STRIP, STRIP), STRIP)
        total = jnp.zeros((8, STRIP), F32)
        for k in range(PEERS):
            total = total + far[k][HALF : HALF + 8, at].astype(F32)
        limit = jnp.floor(total[0:1] / float(CLIP_PARTS))

        def tiles():
            for d in range(PEERS):
                for r in range(0, HALF, 16):
                    yield near_ref[d, r : r + 16, at], near_clipped, near_home[d] + r
                    yield far[d][r : r + 16, at], far_clipped, far_home[d] + r

        def more_above(level):
            near = level.astype(BF).astype(F32)
            above = (level * (1.0 + 2.0**-8)).astype(BF).astype(F32)
            bound = jnp.where(near >= level, near, above)
            bound = jnp.broadcast_to(bound, (16, STRIP)).astype(BF)
            one, nil = jnp.ones_like(bound), jnp.zeros_like(bound)
            sums = [jnp.zeros((16, STRIP), BF)] * 2
            for i, (tile, _, _) in enumerate(tiles()):
                sums[i % 2] = sums[i % 2] + jnp.where(jnp.abs(tile) >= bound, one, nil)
            return jnp.sum((sums[0] + sums[1]).astype(F32), axis=0, keepdims=True) > limit

        def edge_at(at_edge):
            value = jnp.zeros((1, STRIP), F32)
            for j in range(16):
                value = jnp.where(at_edge == float(j), edges[j], value)
            return value

        def coarse(i, found):
            m, step = found
            return jnp.where(more_above(edge_at(m + (step - 1.0))), m + step, m), step * 0.5

        start = jnp.zeros((1, STRIP), F32)
        m, _ = lax.fori_loop(0, 4, coarse, (start, start + 8.0))
        upper, lower = edge_at(m), edge_at(m - 1.0)

        def finer(i, found):
            n, step = found
            level = lower + (upper - lower) * ((n + step) * (1.0 / FINE))
            return jnp.where(more_above(level), n + step, n), step * 0.5

        n, _ = lax.fori_loop(0, 3, finer, (start, start + 4.0))
        scale = jnp.where(n == FINE - 1.0, upper, lower + (upper - lower) * ((n + 1.0) * (1.0 / FINE)))
        top = jnp.broadcast_to(scale, (16, STRIP)).astype(BF)
        for tile, target, row in tiles():
            target[pl.ds(pl.multiple_of(row, 16), 16), at] = jnp.minimum(jnp.maximum(tile, -top), top)
        return carry

    lax.fori_loop(0, width // STRIP, strip, 0)
    for copy in copies:
        copy.wait()
    products(far_clipped, gate_ref, up_ref, outs)


def expert_in(place, edges, gate, up, near, far, count):
    width, hidden = gate.shape
    outs = pl.pallas_call(
        functools.partial(expert_kernel, count),
        in_specs=[whole(SMEM), whole(SMEM), whole(pl.ANY), whole(pl.ANY)] + [whole()] * (1 + PEERS),
        out_specs=[whole()] * 7 + [whole(SMEM)],
        out_shape=product_shapes(hidden) + [shape_of(ROWS, width), jax.ShapeDtypeStruct((1,), F32)],
        scratch_shapes=[
            VMEM((width, hidden), BF),
            VMEM((width, hidden), BF),
            VMEM((ROWS, width), BF),
            pltpu.SemaphoreType.DMA((2,)),
        ],
        name="expert_in",
    )(place, edges, gate, up, near, *far)
    return outs[:6], outs[6], outs[7]


def later_kernel(block_ref, gate_hbm, up_hbm, *refs):
    outs, (gate_ref, up_ref, sems) = refs[:6], refs[6:]
    copies = fetch(gate_hbm, up_hbm, gate_ref, up_ref, sems)
    for copy in copies:
        copy.start()
    for copy in copies:
        copy.wait()
    products(block_ref, gate_ref, up_ref, outs)


def expert_later(block, gate, up):
    width, hidden = gate.shape
    return pl.pallas_call(
        later_kernel,
        in_specs=[whole(), whole(pl.ANY), whole(pl.ANY)],
        out_specs=[whole()] * 6,
        out_shape=product_shapes(hidden),
        scratch_shapes=[
            VMEM((width, hidden), BF),
            VMEM((width, hidden), BF),
            pltpu.SemaphoreType.DMA((2,)),
        ],
        name="expert_later",
    )(block, gate, up)


def down_kernel(split, place_ref, down_ref, *refs):
    outs, all_ref = refs[NX:-1], refs[-1]
    for j in range(NX):
        at = pl.multiple_of(lax.rem(place_ref[0] + j, NX) * SHARE, 16)
        all_ref[pl.ds(at, SHARE), :] = refs[j][...]

    result = jnp.dot(all_ref[...], down_ref[...], preferred_element_type=F32)
    if not split:
        outs[0][...] = result.astype(BF)
        return
    for d in range(PEERS):
        for s in range(2):
            start = d * HALF + s * SPAN
            outs[s][d, :, :] = result[start : start + SPAN, :].astype(BF)


def expert_out(place, down, pieces, split):
    hidden, width = down.shape
    shapes = [shape_of(PEERS, SPAN, width)] * 2 if split else [shape_of(ROWS, width)]
    return pl.pallas_call(
        functools.partial(down_kernel, split),
        in_specs=[whole(SMEM)] + [whole()] * (1 + NX),
        out_specs=[whole()] * len(shapes),
        out_shape=shapes,
        scratch_shapes=[VMEM((ROWS, hidden), BF)],
        name="expert_out",
    )(place, down, *pieces)


def mix_far_kernel(place_ref, first_ref, second_ref, back_ref, *refs):
    outs, held = refs[:-1], refs[-1]
    tok = outs[0].shape[0]
    for s, combine_ref in enumerate((first_ref, second_ref)):
        for k in range(PEERS):
            held[k * SPAN : (k + 1) * SPAN, :] = back_ref[peer(place_ref, k, 1), s * SPAN : (s + 1) * SPAN, :]
        total = jnp.dot(combine_ref[...], held[...], preferred_element_type=F32).astype(BF)
        for i in range(PAIR):
            outs[PAIR * s + i][...] = total[i * tok : (i + 1) * tok, :]


def mix_far(place, combines, back):
    width = back.shape[2]
    tok = combines[0].shape[0] // PAIR
    return pl.pallas_call(
        mix_far_kernel,
        in_specs=[whole(SMEM)] + [whole()] * 3,
        out_specs=[whole()] * (2 * PAIR),
        out_shape=[shape_of(tok, width)] * (2 * PAIR),
        scratch_shapes=[VMEM((LANES, width), BF)],
        name="mix_far",
    )(place, *combines, back)


def mix_kernel(combine_ref, back_ref, *outs):
    tok = outs[0].shape[0]
    total = jnp.dot(combine_ref[...], back_ref[...], preferred_element_type=F32).astype(BF)
    for i in range(PAIR):
        outs[i][...] = total[i * tok : (i + 1) * tok, :]


def mix(combine, back):
    width = back.shape[1]
    tok = combine.shape[0] // PAIR
    return pl.pallas_call(
        mix_kernel,
        in_specs=[whole()] * 2,
        out_specs=[whole()] * PAIR,
        out_shape=[shape_of(tok, width)] * PAIR,
        name="mix",
    )(combine, back)


def ring(value, axis, size, shift):
    if shift % size == 0:
        return value
    return lax.ppermute(value, axis, [(i, (i + shift) % size) for i in range(size)])


def to_peer(value, k):
    if k == 0:
        return value
    dy, dc = k // NC, k % NC
    pairs = [
        (y * NC + c, (y + dy) % NY * NC + (c + dc) % NC) for y in range(NY) for c in range(NC)
    ]
    return lax.ppermute(value, OWNERS, pairs)


def swap_rows(rows):
    back = lax.all_to_all(rows, OWNERS, 0, 0, tiled=True)
    return back


def summed(pieces):
    right, left = pieces[:2]
    return ring(right, "x", NX, 1), ring(left, "x", NX, -1)


def activated(pieces, hops):
    gate_own, up_own, gate_next, up_last = pieces[2:]
    right, left = hops
    gate_sum = (gate_next.astype(F32) + right[:SHARE].astype(F32)).astype(BF)
    up_sum = (up_last.astype(F32) + left[:SHARE].astype(F32)).astype(BF)
    gate_sum = ring(gate_sum, "x", NX, 1)
    up_sum = ring(up_sum, "x", NX, -1)
    gate = gate_own.astype(F32) + gate_sum.astype(F32) + left[SHARE:].astype(F32)
    up = up_own.astype(F32) + up_sum.astype(F32) + right[SHARE:].astype(F32)
    return (jax.nn.silu(gate) * up).astype(BF)


def spread(hidden):
    return [ring(hidden, "x", NX, -j) for j in range(NX)]


def body(tokens, expert_ids, route_weights, gate_weight, up_weight, down_weight, bin_edges):
    tok, width = tokens.shape
    place = jnp.stack([lax.axis_index(a) for a in ("x", "y", "z", "c")]).astype(jnp.int32)
    side = jnp.concatenate([expert_ids.astype(BF), route_weights], axis=1)
    side = jnp.pad(side, ((0, 0), (0, META - side.shape[1])))
    wide = jnp.concatenate([tokens, side], axis=1)
    near_offsets = [o for pair in NEAR for o in pair]
    far_offsets = [o for pair in FAR for o in pair]
    near_blocks = [ring(wide, "z", NZ, -o) for o in near_offsets]
    far_blocks = [ring(wide, "z", NZ, -o) for o in far_offsets]
    (rows,), near_maps = dispatch(place, near_blocks, [])
    near = swap_rows(rows)
    rows, far_maps = dispatch(place, far_blocks, near_blocks)
    far = [to_peer(r, k) for k, r in enumerate(rows)]
    gate, up, down = gate_weight[0], up_weight[0], down_weight[0]
    far_pieces, clipped, expert_load = expert_in(
        place, bin_edges, gate, up, near, far, tok * expert_ids.shape[1]
    )
    far_hops = summed(far_pieces)
    near_pieces = expert_later(clipped, gate, up)
    hidden = activated(far_pieces, far_hops)
    near_hops = summed(near_pieces)
    shares = spread(hidden)
    (result,) = expert_out(place, down, shares, False)
    far_back = swap_rows(result.reshape(PEERS, HALF, width))
    hidden = activated(near_pieces, near_hops)
    shares = spread(hidden)
    results = expert_out(place, down, shares, True)
    second_back = swap_rows(results[1]).reshape(LANES, width)
    first_back = swap_rows(results[0]).reshape(LANES, width)
    sums = mix_far(place, far_maps, far_back)
    sums = [ring(part, "z", NZ, o) for o, part in zip(far_offsets, sums)]
    more = mix(near_maps[1], second_back)
    sums += [ring(part, "z", NZ, o) for o, part in zip(NEAR[1], more)]
    more = mix(near_maps[0], first_back)
    sums += [ring(part, "z", NZ, o) for o, part in zip(NEAR[0], more)]
    total = sums[0].astype(F32)
    for part in sums[1:]:
        total = total + part.astype(F32)
    return (total.astype(BF), expert_load)


def solution(mesh):
    finer = Mesh(mesh.devices.reshape(NY, NZ, NC, NX), ("y", "z", "c", "x"))
    placed = (
        P(EXPERT, "x"),
        P(EXPERT, None),
        P(EXPERT, None),
        P(EXPERT, "x", None),
        P(EXPERT, "x", None),
        P(EXPERT, None, "x"),
        P(),
    )
    return jax.shard_map(
        body,
        mesh=finer,
        in_specs=placed,
        out_specs=(P(EXPERT, "x"), P(EXPERT)),
        check_vma=False,
    )
```

```python
import functools

import jax
import jax.numpy as jnp
import numpy as np
from jax import lax
from jax.experimental import pallas as pl
from jax.experimental.pallas import tpu as pltpu
from jax.sharding import Mesh
from jax.sharding import PartitionSpec as P


FINE = 8
CLIP_PARTS = 8
CAP = 12
META = 128
NY, NZ, NC, NX = 4, 8, 2, 4
PEERS = NY * NC
EXPERT = ("y", "z", "c")
OWNERS = ("y", "c")
NEAR = ((0, 1), (7, 2))
FAR = ((6, 3), (5, 4))
PAIR = 2
SPAN = CAP * PAIR
LANES = PEERS * SPAN
HALF = SPAN * PAIR
ROWS = PEERS * HALF
SHARE = ROWS // NX
STRIP = 256
WIDE = 512

BF = jnp.bfloat16
F32 = jnp.float32
VMEM = pltpu.VMEM
SMEM = pltpu.SMEM


def whole(space=VMEM):
    return pl.BlockSpec(memory_space=space)


def shape_of(*shape):
    return jax.ShapeDtypeStruct(shape, BF)


def lane_table():
    lane = np.arange(LANES)
    table = np.zeros((8, LANES), np.float32)
    table[0] = lane // SPAN // NC
    table[1] = lane // SPAN % NC
    table[2] = lane % SPAN // CAP
    table[3] = lane % CAP
    return table


def peer(place, k, sign):
    dy, dc = k // NC, k % NC
    core = place[3] if dc == 0 else 1 - place[3]
    return lax.rem(place[1] + sign * dy + NY, NY) * NC + core


def dispatch_kernel(relative, place_ref, table_ref, *refs):
    tok = refs[0].shape[0]
    width = refs[0].shape[1] - META
    blocks = refs[: 2 * PAIR]
    extra = refs[2 * PAIR : 2 * PAIR + (2 * PAIR if relative else 0)]
    outs = refs[len(blocks) + len(extra) :]
    rows_refs, combine_refs, (map_ref, tokens_ref) = outs[:-4], outs[-4:-2], outs[-2:]

    def numbers(y, core):
        if relative:
            y = y + place_ref[1].astype(F32)
            y = jnp.where(y >= float(NY), y - float(NY), y)
            own = place_ref[3].astype(F32)
            core = own + core - 2.0 * own * core
        return y * float(NZ * NC) + core + place_ref[2].astype(F32) * float(NC)

    expert = numbers(table_ref[0:1, :], table_ref[1:2, :])
    spot = table_ref[2:3, :]
    rank_wanted = table_ref[3:4, :]
    row = lax.broadcasted_iota(jnp.int32, (tok, tok), 0)
    col = lax.broadcasted_iota(jnp.int32, (tok, tok), 1)
    before = jnp.where(col < row, 1.0, 0.0).astype(BF)
    for s in range(2):
        for i in range(PAIR):
            block = blocks[PAIR * s + i]
            meta = block[:, width : width + META].astype(F32)
            hit = jnp.zeros((tok, LANES), F32)
            weight = jnp.zeros((tok, LANES), F32)
            for k in range(8):
                same = meta[:, k : k + 1] == expert
                hit = jnp.where(same, 1.0, hit)
                weight = jnp.where(same, meta[:, 8 + k : 9 + k], weight)
            rank = jnp.dot(before, hit.astype(BF), preferred_element_type=F32)
            chosen = (hit > 0.0) & (rank == rank_wanted) & (spot == float(i))
            map_ref[i * tok : (i + 1) * tok, :] = jnp.where(chosen, 1.0, 0.0).astype(BF)
            combine_refs[s][i * tok : (i + 1) * tok, :] = jnp.where(chosen, weight, 0.0).astype(BF)
            tokens_ref[i * tok : (i + 1) * tok, :] = block[:, :width]
        rows = lax.dot_general(
            map_ref[...], tokens_ref[...], (((0,), (0,)), ((), ())), preferred_element_type=F32
        )
        for d in range(PEERS):
            part = rows[d * SPAN : (d + 1) * SPAN, :].astype(BF)
            if relative:
                rows_refs[d][s * SPAN : (s + 1) * SPAN, :] = part
            else:
                rows_refs[0][d, s * SPAN : (s + 1) * SPAN, :] = part
    if relative:
        lane = lax.broadcasted_iota(jnp.int32, (1, META), 1)
        peer_expert = numbers((lane // NC).astype(F32), (lane % NC).astype(F32))
        named = jnp.zeros((1, META), F32)
        load = jnp.zeros((1, META), F32)
        metas = [b[:, width : width + META] for b in blocks] + [b[...] for b in extra]
        for meta in metas:
            meta = meta.astype(F32)
            for k in range(8):
                same = meta[:, k : k + 1] == peer_expert
                named = named + jnp.sum(jnp.where(same, 1.0, 0.0), axis=0, keepdims=True)
                load = load + jnp.sum(
                    jnp.where(same, meta[:, 8 + k : 9 + k], 0.0), axis=0, keepdims=True
                )
        high = load.astype(BF).astype(F32)
        middle = (load - high).astype(BF).astype(F32)
        low = load - high - middle
        line = lax.broadcasted_iota(jnp.int32, (8, META), 0)
        pieces = jnp.where(line == 2, middle, jnp.where(line == 3, low, 0.0))
        pieces = jnp.where(line == 0, named, jnp.where(line == 1, high, pieces))
        for d in range(PEERS):
            rows_refs[d][HALF : HALF + 8, :] = jnp.broadcast_to(pieces[:, d : d + 1], (8, width)).astype(BF)


def dispatch(place, blocks, extra):
    tok, wide = blocks[0].shape
    width = wide - META
    side = pl.BlockSpec((tok, META), lambda i: (0, width // META))
    full = pl.BlockSpec((tok, wide), lambda i: (0, 0))
    flat = pl.BlockSpec((PAIR * tok, LANES), lambda i: (0, 0))
    if extra:
        specs = [pl.BlockSpec((HALF + 8, width), lambda i: (0, 0))] * PEERS
        shapes = [shape_of(HALF + 8, width)] * PEERS
    else:
        specs = [pl.BlockSpec((PEERS, HALF, width), lambda i: (0, 0, 0))]
        shapes = [shape_of(PEERS, HALF, width)]
    outs = pl.pallas_call(
        functools.partial(dispatch_kernel, bool(extra)),
        grid=(1,),
        in_specs=[whole(SMEM), pl.BlockSpec((8, LANES), lambda i: (0, 0))]
        + [full] * len(blocks)
        + [side] * len(extra),
        out_specs=specs + [flat] * 2,
        out_shape=shapes + [shape_of(PAIR * tok, LANES)] * 2,
        scratch_shapes=[VMEM((PAIR * tok, LANES), BF), VMEM((PAIR * tok, width), BF)],
        name="dispatch",
    )(place, jnp.asarray(lane_table()), *blocks, *extra)
    return outs[:-2], outs[-2:]


def products(block_ref, gate_ref, up_ref, outs):
    right, left, gate_own, up_own, gate_next, up_last = outs

    def columns(n, carry):
        at = pl.ds(pl.multiple_of(n * WIDE, WIDE), WIDE)
        gate = jnp.dot(block_ref[...], gate_ref[:, at], preferred_element_type=F32).astype(BF)
        right[:SHARE, at] = gate[2 * SHARE : 3 * SHARE, :]
        left[SHARE:, at] = gate[3 * SHARE :, :]
        gate_own[:, at] = gate[:SHARE, :]
        gate_next[:, at] = gate[SHARE : 2 * SHARE, :]
        up = jnp.dot(block_ref[...], up_ref[:, at], preferred_element_type=F32).astype(BF)
        left[:SHARE, at] = up[2 * SHARE : 3 * SHARE, :]
        right[SHARE:, at] = up[SHARE : 2 * SHARE, :]
        up_own[:, at] = up[:SHARE, :]
        up_last[:, at] = up[3 * SHARE :, :]
        return carry

    lax.fori_loop(0, gate_ref.shape[1] // WIDE, columns, 0)


def product_shapes(hidden):
    return [shape_of(2 * SHARE, hidden)] * 2 + [shape_of(SHARE, hidden)] * 4


def fetch(gate_hbm, up_hbm, gate_ref, up_ref, sems):
    return [
        pltpu.make_async_copy(gate_hbm, gate_ref, sems.at[0]),
        pltpu.make_async_copy(up_hbm, up_ref, sems.at[1]),
    ]


def expert_kernel(count, place_ref, edges_ref, gate_hbm, up_hbm, near_ref, *refs):
    far = refs[:PEERS]
    outs = refs[PEERS : PEERS + 6]
    near_clipped, load_ref = refs[PEERS + 6 : PEERS + 8]
    gate_ref, up_ref, far_clipped, sems = refs[PEERS + 8 :]
    width = far_clipped.shape[1]
    copies = fetch(gate_hbm, up_hbm, gate_ref, up_ref, sems)
    for copy in copies:
        copy.start()
    edges = [edges_ref[j] for j in range(16)]
    load = jnp.zeros((8, 128), F32)
    for k in range(PEERS):
        load = load + far[k][HALF : HALF + 8, 0:128].astype(F32)
    load = (load[1:2] + load[2:3] + load[3:4]) / float(count)
    load_ref[0] = load[0, 0]

    def home(d):
        turn = lax.rem(d // NC - place_ref[0] + NX, NX)
        return turn * SHARE + lax.rem(d, NC) * HALF

    near_home = [home(d) for d in range(PEERS)]
    far_home = [home(peer(place_ref, k, -1)) for k in range(PEERS)]

    def strip(s, carry):
        at = pl.ds(pl.multiple_of(s * STRIP, STRIP), STRIP)
        total = jnp.zeros((8, STRIP), F32)
        for k in range(PEERS):
            total = total + far[k][HALF : HALF + 8, at].astype(F32)
        limit = jnp.floor(total[0:1] / float(CLIP_PARTS))

        def tiles():
            for d in range(PEERS):
                for r in range(0, HALF, 16):
                    yield near_ref[d, r : r + 16, at], near_clipped, near_home[d] + r
                    yield far[d][r : r + 16, at], far_clipped, far_home[d] + r

        def more_above(level):
            near = level.astype(BF).astype(F32)
            above = (level * (1.0 + 2.0**-8)).astype(BF).astype(F32)
            bound = jnp.where(near >= level, near, above)
            bound = jnp.broadcast_to(bound, (16, STRIP)).astype(BF)
            one, nil = jnp.ones_like(bound), jnp.zeros_like(bound)
            sums = [jnp.zeros((16, STRIP), BF)] * 2
            for i, (tile, _, _) in enumerate(tiles()):
                sums[i % 2] = sums[i % 2] + jnp.where(jnp.abs(tile) >= bound, one, nil)
            return jnp.sum((sums[0] + sums[1]).astype(F32), axis=0, keepdims=True) > limit

        def edge_at(at_edge):
            value = jnp.zeros((1, STRIP), F32)
            for j in range(16):
                value = jnp.where(at_edge == float(j), edges[j], value)
            return value

        def coarse(i, found):
            m, step = found
            return jnp.where(more_above(edge_at(m + (step - 1.0))), m + step, m), step * 0.5

        start = jnp.zeros((1, STRIP), F32)
        m, _ = lax.fori_loop(0, 4, coarse, (start, start + 8.0))
        upper, lower = edge_at(m), edge_at(m - 1.0)

        def finer(i, found):
            n, step = found
            level = lower + (upper - lower) * ((n + step) * (1.0 / FINE))
            return jnp.where(more_above(level), n + step, n), step * 0.5

        n, _ = lax.fori_loop(0, 3, finer, (start, start + 4.0))
        scale = jnp.where(n == FINE - 1.0, upper, lower + (upper - lower) * ((n + 1.0) * (1.0 / FINE)))
        top = jnp.broadcast_to(scale, (16, STRIP)).astype(BF)
        for tile, target, row in tiles():
            target[pl.ds(pl.multiple_of(row, 16), 16), at] = jnp.minimum(jnp.maximum(tile, -top), top)
        return carry

    lax.fori_loop(0, width // STRIP, strip, 0)
    for copy in copies:
        copy.wait()
    products(far_clipped, gate_ref, up_ref, outs)


def expert_in(place, edges, gate, up, near, far, count):
    width, hidden = gate.shape
    outs = pl.pallas_call(
        functools.partial(expert_kernel, count),
        in_specs=[whole(SMEM), whole(SMEM), whole(pl.ANY), whole(pl.ANY)] + [whole()] * (1 + PEERS),
        out_specs=[whole()] * 7 + [whole(SMEM)],
        out_shape=product_shapes(hidden) + [shape_of(ROWS, width), jax.ShapeDtypeStruct((1,), F32)],
        scratch_shapes=[
            VMEM((width, hidden), BF),
            VMEM((width, hidden), BF),
            VMEM((ROWS, width), BF),
            pltpu.SemaphoreType.DMA((2,)),
        ],
        name="expert_in",
    )(place, edges, gate, up, near, *far)
    return outs[:6], outs[6], outs[7]


def later_kernel(block_ref, gate_hbm, up_hbm, *refs):
    outs, (gate_ref, up_ref, sems) = refs[:6], refs[6:]
    copies = fetch(gate_hbm, up_hbm, gate_ref, up_ref, sems)
    for copy in copies:
        copy.start()
    for copy in copies:
        copy.wait()
    products(block_ref, gate_ref, up_ref, outs)


def expert_later(block, gate, up):
    width, hidden = gate.shape
    return pl.pallas_call(
        later_kernel,
        in_specs=[whole(), whole(pl.ANY), whole(pl.ANY)],
        out_specs=[whole()] * 6,
        out_shape=product_shapes(hidden),
        scratch_shapes=[
            VMEM((width, hidden), BF),
            VMEM((width, hidden), BF),
            pltpu.SemaphoreType.DMA((2,)),
        ],
        name="expert_later",
    )(block, gate, up)


def down_kernel(split, place_ref, down_ref, *refs):
    outs, all_ref = refs[NX:-1], refs[-1]

    @pl.when(pl.program_id(0) == 0)
    def _():
        for j in range(NX):
            at = pl.multiple_of(lax.rem(place_ref[0] + j, NX) * SHARE, 16)
            all_ref[pl.ds(at, SHARE), :] = refs[j][...]

    result = jnp.dot(all_ref[...], down_ref[...], preferred_element_type=F32)
    if not split:
        outs[0][...] = result.astype(BF)
        return
    for d in range(PEERS):
        for s in range(2):
            start = d * HALF + s * SPAN
            outs[s][d, :, :] = result[start : start + SPAN, :].astype(BF)


def expert_out(place, down, pieces, split):
    hidden, width = down.shape
    part = width // 2
    if split:
        shapes = [shape_of(PEERS, SPAN, width)] * 2
        specs = [pl.BlockSpec((PEERS, SPAN, part), lambda j: (0, 0, j))] * 2
    else:
        shapes = [shape_of(ROWS, width)]
        specs = [pl.BlockSpec((ROWS, part), lambda j: (0, j))]
    return pl.pallas_call(
        functools.partial(down_kernel, split),
        grid=(2,),
        in_specs=[whole(SMEM), pl.BlockSpec((hidden, part), lambda j: (0, j))]
        + [pl.BlockSpec((SHARE, hidden), lambda j: (0, 0))] * NX,
        out_specs=specs,
        out_shape=shapes,
        scratch_shapes=[VMEM((ROWS, hidden), BF)],
        name="expert_out",
    )(place, down, *pieces)


def mix_far_kernel(place_ref, first_ref, second_ref, back_ref, *refs):
    outs, held = refs[:-1], refs[-1]
    tok = outs[0].shape[0]
    for s, combine_ref in enumerate((first_ref, second_ref)):
        for k in range(PEERS):
            held[k * SPAN : (k + 1) * SPAN, :] = back_ref[peer(place_ref, k, 1), s * SPAN : (s + 1) * SPAN, :]
        total = jnp.dot(combine_ref[...], held[...], preferred_element_type=F32).astype(BF)
        for i in range(PAIR):
            outs[PAIR * s + i][...] = total[i * tok : (i + 1) * tok, :]


def mix_far(place, combines, back):
    width = back.shape[2]
    tok = combines[0].shape[0] // PAIR
    return pl.pallas_call(
        mix_far_kernel,
        in_specs=[whole(SMEM)] + [whole()] * 3,
        out_specs=[whole()] * (2 * PAIR),
        out_shape=[shape_of(tok, width)] * (2 * PAIR),
        scratch_shapes=[VMEM((LANES, width), BF)],
        name="mix_far",
    )(place, *combines, back)


def mix_kernel(combine_ref, back_ref, *outs):
    tok = outs[0].shape[0]
    total = jnp.dot(combine_ref[...], back_ref[...], preferred_element_type=F32).astype(BF)
    for i in range(PAIR):
        outs[i][...] = total[i * tok : (i + 1) * tok, :]


def mix(combine, back):
    width = back.shape[1]
    tok = combine.shape[0] // PAIR
    return pl.pallas_call(
        mix_kernel,
        in_specs=[whole()] * 2,
        out_specs=[whole()] * PAIR,
        out_shape=[shape_of(tok, width)] * PAIR,
        name="mix",
    )(combine, back)


def ring(value, axis, size, shift):
    if shift % size == 0:
        return value
    return lax.ppermute(value, axis, [(i, (i + shift) % size) for i in range(size)])


def to_peer(value, k):
    if k == 0:
        return value
    dy, dc = k // NC, k % NC
    pairs = [
        (y * NC + c, (y + dy) % NY * NC + (c + dc) % NC) for y in range(NY) for c in range(NC)
    ]
    return lax.ppermute(value, OWNERS, pairs)


def swap_rows(rows):
    back = lax.all_to_all(rows, OWNERS, 0, 0, tiled=True)
    return back


def summed(pieces):
    right, left = pieces[:2]
    return ring(right, "x", NX, 1), ring(left, "x", NX, -1)


def activated(pieces, hops):
    gate_own, up_own, gate_next, up_last = pieces[2:]
    right, left = hops
    gate_sum = (gate_next.astype(F32) + right[:SHARE].astype(F32)).astype(BF)
    up_sum = (up_last.astype(F32) + left[:SHARE].astype(F32)).astype(BF)
    gate_sum = ring(gate_sum, "x", NX, 1)
    up_sum = ring(up_sum, "x", NX, -1)
    gate = gate_own.astype(F32) + gate_sum.astype(F32) + left[SHARE:].astype(F32)
    up = up_own.astype(F32) + up_sum.astype(F32) + right[SHARE:].astype(F32)
    return (jax.nn.silu(gate) * up).astype(BF)


def spread(hidden):
    return [ring(hidden, "x", NX, -j) for j in range(NX)]


def body(tokens, expert_ids, route_weights, gate_weight, up_weight, down_weight, bin_edges):
    tok, width = tokens.shape
    place = jnp.stack([lax.axis_index(a) for a in ("x", "y", "z", "c")]).astype(jnp.int32)
    side = jnp.concatenate([expert_ids.astype(BF), route_weights], axis=1)
    side = jnp.pad(side, ((0, 0), (0, META - side.shape[1])))
    wide = jnp.concatenate([tokens, side], axis=1)
    near_offsets = [o for pair in NEAR for o in pair]
    far_offsets = [o for pair in FAR for o in pair]
    near_blocks = [ring(wide, "z", NZ, -o) for o in near_offsets]
    far_blocks = [ring(wide, "z", NZ, -o) for o in far_offsets]
    (rows,), near_maps = dispatch(place, near_blocks, [])
    near = swap_rows(rows)
    rows, far_maps = dispatch(place, far_blocks, near_blocks)
    far = [to_peer(r, k) for k, r in enumerate(rows)]
    gate, up, down = gate_weight[0], up_weight[0], down_weight[0]
    far_pieces, clipped, expert_load = expert_in(
        place, bin_edges, gate, up, near, far, tok * expert_ids.shape[1]
    )
    far_hops = summed(far_pieces)
    near_pieces = expert_later(clipped, gate, up)
    hidden = activated(far_pieces, far_hops)
    near_hops = summed(near_pieces)
    shares = spread(hidden)
    (result,) = expert_out(place, down, shares, False)
    far_back = swap_rows(result.reshape(PEERS, HALF, width))
    hidden = activated(near_pieces, near_hops)
    shares = spread(hidden)
    results = expert_out(place, down, shares, True)
    second_back = swap_rows(results[1]).reshape(LANES, width)
    first_back = swap_rows(results[0]).reshape(LANES, width)
    sums = mix_far(place, far_maps, far_back)
    sums = [ring(part, "z", NZ, o) for o, part in zip(far_offsets, sums)]
    more = mix(near_maps[1], second_back)
    sums += [ring(part, "z", NZ, o) for o, part in zip(NEAR[1], more)]
    more = mix(near_maps[0], first_back)
    sums += [ring(part, "z", NZ, o) for o, part in zip(NEAR[0], more)]
    total = sums[0].astype(F32)
    for part in sums[1:]:
        total = total + part.astype(F32)
    return (total.astype(BF), expert_load)


def solution(mesh):
    finer = Mesh(mesh.devices.reshape(NY, NZ, NC, NX), ("y", "z", "c", "x"))
    placed = (
        P(EXPERT, "x"),
        P(EXPERT, None),
        P(EXPERT, None),
        P(EXPERT, "x", None),
        P(EXPERT, "x", None),
        P(EXPERT, None, "x"),
        P(),
    )
    return jax.shard_map(
        body,
        mesh=finer,
        in_specs=placed,
        out_specs=(P(EXPERT, "x"), P(EXPERT)),
        check_vma=False,
    )
```
